32 devices in a mesh: dp: 4 (over y, z), wg: 8 (over x, core).
Axes of the slice: x: 4, y: 2, z: 2, core: 2. Of those that a mesh axis runs over, the one named last changes fastest.
The devices are a block of a 4x4x8 slice.
Arguments:
- hidden: bfloat16 [32768, 1024], P(('dp', 'wg')), parts along dimension 0
- choice: int32 [32768, 8], P(('dp', 'wg')), parts along dimension 0
- pre_scale: float32 [1024], replicated
- w_router: bfloat16 [1024, 32], replicated
- w_gelu: bfloat16 [32, 1024, 512], P(None, None, 'wg')
- w_linear: bfloat16 [32, 1024, 512], P(None, None, 'wg')
- w_down: bfloat16 [32, 512, 1024], P(None, 'wg')
- post_scale: float32 [1024], replicated
Outputs:
- output: bfloat16 [32768, 1024], P(('dp', 'wg')), parts along dimension 0
There are 4 independent parts. The reference program is written for one: setup_inputs(seed, part) draws one part's arguments, and reference() takes and returns one part's arrays. A program takes and returns all parts, laid end to end along the dimension named above; an argument that names none is the same for every part.
All inputs are finite; a program needn't handle non-finite values.
Results may differ from the reference program's by a relative error of at most 0.001.
Values are sent between devices in bfloat16 or wider.
A program may use at most 768 MiB of HBM per device.

```python
import jax
import jax.numpy as jnp
from jax import lax

D_MODEL = 1024
D_FF = 512
EXPERTS = 32
TOP_K = 8
TOKENS_DEV = 1024
GROUP_DEVS = 8
EPS = 1e-5


def block_choice(block_key):
    mean_load = TOKENS_DEV * TOP_K // EXPERTS
    key_perm, key_delta, key_rows = jax.random.split(block_key, 3)
    expert_perm = jax.random.permutation(key_perm, EXPERTS)
    pair_delta = jax.random.randint(key_delta, (EXPERTS,), 0, mean_load)
    position = jnp.arange(EXPERTS)
    pair_index = jnp.maximum((position - 3) // 2, 0)
    pair_sign = jnp.where((position - 3) % 2 == 0, 1, -1)
    paired = (position >= 3) & (4 + 2 * pair_index < EXPERTS)
    load_delta = jnp.where(paired, pair_sign * pair_delta[pair_index], 0)
    load_delta = load_delta + jnp.where(position == 0, mean_load, 0) - jnp.where((position == 1) | (position == 2), mean_load // 2, 0)
    expert_loads = mean_load + load_delta
    run_ends = jnp.cumsum(expert_loads)
    flat_pos = jnp.arange(TOKENS_DEV * TOP_K)
    run_index = jnp.sum((flat_pos[:, None] >= run_ends[None, :]).astype(jnp.int32), axis=1)
    choice_grid = expert_perm[run_index].reshape(TOP_K, TOKENS_DEV).T
    row_perm = jax.random.permutation(key_rows, TOKENS_DEV)
    return choice_grid[row_perm].astype(jnp.int32)


def setup_inputs(seed: int = 0, part: int = 0) -> dict:
    weight_keys = jax.random.split(jax.random.key(seed), 6)
    part_key = jax.random.fold_in(jax.random.key(seed + 1), part)
    key_hidden, key_choice = jax.random.split(part_key)
    row_count = GROUP_DEVS * TOKENS_DEV
    hidden = jax.random.normal(key_hidden, (row_count, D_MODEL), jnp.float32).astype(jnp.bfloat16)
    choice = jax.vmap(block_choice)(jax.random.split(key_choice, GROUP_DEVS)).reshape(row_count, TOP_K)
    pre_scale = 1.0 + 0.5 * jax.random.normal(weight_keys[0], (D_MODEL,), jnp.float32)
    w_router = (jax.random.normal(weight_keys[1], (D_MODEL, EXPERTS), jnp.float32) * D_MODEL ** -0.5).astype(jnp.bfloat16)
    w_gelu = (jax.random.normal(weight_keys[2], (EXPERTS, D_MODEL, D_FF), jnp.float32) * D_MODEL ** -0.5).astype(jnp.bfloat16)
    w_linear = (jax.random.normal(weight_keys[3], (EXPERTS, D_MODEL, D_FF), jnp.float32) * D_MODEL ** -0.5).astype(jnp.bfloat16)
    w_down = (jax.random.normal(weight_keys[4], (EXPERTS, D_FF, D_MODEL), jnp.float32) * D_FF ** -0.5).astype(jnp.bfloat16)
    post_scale = 1.0 + 0.5 * jax.random.normal(weight_keys[5], (D_MODEL,), jnp.float32)
    return dict(hidden=hidden, choice=choice, pre_scale=pre_scale, w_router=w_router, w_gelu=w_gelu, w_linear=w_linear, w_down=w_down, post_scale=post_scale)


def rms_norm(values, gain_vec):
    return values * lax.rsqrt(jnp.mean(values * values, axis=-1, keepdims=True) + EPS) * gain_vec


def route_slots(block_ids, capacity):
    tok_rows, top_k = block_ids.shape
    flat_ids = block_ids.reshape(-1)
    sort_order = jnp.argsort(flat_ids, stable=True)
    counts = jnp.sum((flat_ids[:, None] == jnp.arange(EXPERTS)[None, :]).astype(jnp.int32), axis=0)
    starts = jnp.cumsum(counts) - counts
    slot_rank = jnp.arange(capacity)
    source = jnp.minimum(starts[:, None] + slot_rank[None, :], tok_rows * top_k - 1)
    slot_token = sort_order[source].reshape(-1) // top_k
    sorted_pos = jnp.argsort(sort_order, stable=True)
    slot_of = flat_ids * capacity + sorted_pos - starts[flat_ids]
    return slot_token, slot_of


def reference(hidden, choice, pre_scale, w_router, w_gelu, w_linear, w_down, post_scale):
    capacity = 2 * TOKENS_DEV * TOP_K // EXPERTS
    hidden_f = hidden.astype(jnp.float32)
    normed = rms_norm(hidden_f, pre_scale).astype(jnp.bfloat16)
    router_probs = jax.nn.softmax(jnp.dot(normed, w_router, preferred_element_type=jnp.float32), axis=-1)
    gate_vals = jnp.take_along_axis(router_probs, choice, axis=1)

    def one_expert(expert_args):
        expert_rows, gelu_w, linear_w, down_w = expert_args
        gelu_in = jnp.dot(expert_rows, gelu_w, preferred_element_type=jnp.float32)
        linear_in = jnp.dot(expert_rows, linear_w, preferred_element_type=jnp.float32)
        hidden_act = (jax.nn.gelu(gelu_in, approximate=True) * linear_in).astype(jnp.bfloat16)
        return jnp.dot(hidden_act, down_w, preferred_element_type=jnp.float32)

    def one_block(block_args):
        block_rows, block_ids, block_gates = block_args
        slot_token, slot_of = route_slots(block_ids, capacity)
        dispatched = jnp.take(block_rows, slot_token, axis=0).reshape(EXPERTS, capacity, D_MODEL)
        expert_out = lax.map(one_expert, (dispatched, w_gelu, w_linear, w_down)).reshape(EXPERTS * capacity, D_MODEL)
        picked = jnp.take(expert_out, slot_of, axis=0).reshape(TOKENS_DEV, TOP_K, D_MODEL)
        return jnp.sum(picked * block_gates[:, :, None], axis=1)

    mixed_out = lax.map(one_block, (normed.reshape(GROUP_DEVS, TOKENS_DEV, D_MODEL), choice.reshape(GROUP_DEVS, TOKENS_DEV, TOP_K), gate_vals.reshape(GROUP_DEVS, TOKENS_DEV, TOP_K))).reshape(GROUP_DEVS * TOKENS_DEV, D_MODEL)
    return (hidden_f + rms_norm(mixed_out, post_scale)).astype(jnp.bfloat16)
```

```python
import functools
import jax
import jax.numpy as jnp
from jax import lax
from jax.experimental import pallas as pl
from jax.experimental.pallas import tpu as pltpu
from jax.sharding import PartitionSpec as P

EPS = 1e-5
KG = 0.7978845608028654
KC = KG * 0.044715
SB = 4
LANES = 128
f32, bf16 = jnp.float32, jnp.bfloat16


def gated_act(u, v, gate):
    w = u * (u * u * KC + KG)
    g = u * (0.5 * jnp.tanh(w) + 0.5)
    a = (g * v).astype(bf16).astype(f32)
    ga = jnp.where(gate >= 0, a * gate, 0.0)
    hi = ga.astype(bf16)
    return hi, (ga - hi.astype(f32)).astype(bf16)


def kernel(n, hid, cht, pre, wr, wu_own, wd_own, post, out, fin,
           wu, wd, xr, chs, xb, gts, u0, u1, h0, h1, l0, l1, ys, rel,
           lsem, asem, arem, wsem, wrem, ssem, srem):
    M, D = xb.shape
    NB = wu.shape[0]
    half = NB // 2
    NI = NB // SB
    me = lax.axis_index('wg')
    right, left = lax.rem(me + 2, n), lax.rem(me + n - 2, n)
    mate = me + 1 - 2 * lax.rem(me, 2)

    barrier = pltpu.get_barrier_semaphore()
    for d in (left, right, mate):
        pl.semaphore_signal(barrier, inc=1, device_id={'wg': d}, device_id_type=pl.DeviceIdType.MESH)
    pl.semaphore_wait(barrier, 3)

    def remote(src, dst, ss, rs, dev):
        return pltpu.make_async_remote_copy(src_ref=src, dst_ref=dst, send_sem=ss, recv_sem=rs,
                                            device_id={'wg': dev}, device_id_type=pl.DeviceIdType.MESH)

    hid_a, hid_b = hid.at[pl.ds(0, M)], hid.at[pl.ds(M, M)]

    def gather(k):
        x_src, c_src, dst, dev = (
            (hid_a, cht.at[0], 1, right), (hid_b, cht.at[1], 2, left),
            (xr.at[1], chs.at[1], 4, right), (xr.at[2], chs.at[2], 3, left),
            (hid_a, cht.at[0], 6, left), (hid_b, cht.at[1], 5, right))[k]
        return (remote(c_src, chs.at[dst], asem.at[2 * k], arem.at[2 * k], dev),
                remote(x_src, xr.at[dst], asem.at[2 * k + 1], arem.at[2 * k + 1], dev))

    def weight(k):
        b, r = half // 4, half // 4 * LANES
        return (remote(wu_own.at[pl.ds(k * b, b)], wu.at[pl.ds(half + k * b, b)], wsem.at[2 * k], wrem.at[2 * k], mate),
                remote(wd_own.at[pl.ds(k * r, r)], wd.at[pl.ds(half * LANES + k * r, r)], wsem.at[2 * k + 1], wrem.at[2 * k + 1], mate))

    def partial(k):
        src, dst, dev = (
            (ys.at[1], fin.at[0], left), (ys.at[2], fin.at[1], right),
            (ys.at[3], rel.at[0], left), (ys.at[4], rel.at[1], right),
            (ys.at[1], fin.at[2], left), (ys.at[2], fin.at[3], right))[k]
        return remote(src, dst, ssem.at[k], srem.at[k], dev)

    for k in (0, 1, 5, 4):
        for c in gather(k):
            c.start()
    for k in range(4):
        for c in weight(k):
            c.start()
    local = [pltpu.make_async_copy(hid_a, xr.at[0], lsem.at[0]),
             pltpu.make_async_copy(cht.at[0], chs.at[0], lsem.at[1]),
             pltpu.make_async_copy(wu_own, wu.at[pl.ds(0, half)], lsem.at[2]),
             pltpu.make_async_copy(wd_own, wd.at[pl.ds(0, half * LANES)], lsem.at[3]),
             pltpu.make_async_copy(hid_b, xr.at[7], lsem.at[4]),
             pltpu.make_async_copy(cht.at[1], chs.at[7], lsem.at[5])]
    for c in local:
        c.start()
    for c in local:
        c.wait()

    us, hs, ls = (u0, u1), (h0, h1), (l0, l1)

    def norm(c):
        @pl.loop(0, M // 64)
        def _(t):
            rows = pl.ds(pl.multiple_of(t * 64, 64), 64)
            x = xr[c, rows].astype(f32)
            xb[rows] = (x * lax.rsqrt(jnp.mean(x * x, axis=-1, keepdims=True) + EPS) * pre[...]).astype(bf16)

    def gates(c):
        E = wr.shape[1]
        logits = jnp.dot(xb[...], wr[...], preferred_element_type=f32)
        e = jnp.exp(logits - logits.max(-1, keepdims=True))
        p = e / e.sum(-1, keepdims=True)
        ch = chs[c]
        ids = lax.broadcasted_iota(jnp.int32, (E, M), 0)
        hit = ch[0:1] == ids
        for j in range(1, ch.shape[0]):
            hit = hit | (ch[j:j + 1] == ids)
        eye = jnp.where(lax.broadcasted_iota(jnp.int32, (E, E), 0) == lax.broadcasted_iota(jnp.int32, (E, E), 1), 1.0, 0.0)
        mask = lax.dot_general(jnp.where(hit, 1.0, 0.0).astype(bf16), eye.astype(bf16), (((0,), (0,)), ((), ())),
                               preferred_element_type=f32)
        g = jnp.where(mask > 0.5, p, -1.0)
        low = lax.broadcasted_iota(jnp.int32, (M, LANES), 1) < LANES // 2
        for q in range(E // 2):
            gts[q] = jnp.where(low, g[:, 2 * q:2 * q + 1], g[:, 2 * q + 1:2 * q + 2])

    def slot(c):
        return c - 4 * (c // 5)

    def up(i, p):
        b = lax.rem(i, NI) * SB
        for k in range(SB):
            us[p][:, k * 256:(k + 1) * 256] = jnp.dot(xb[...], wu[b + k], preferred_element_type=f32)

    def act(i, p):
        b = lax.rem(i * SB, half)
        for k in range(SB):
            hi, lo = gated_act(us[p][:, k * 256:k * 256 + 128], us[p][:, k * 256 + 128:(k + 1) * 256], gts[b + k])
            hs[p][:, k * 128:(k + 1) * 128] = hi
            ls[p][:, k * 128:(k + 1) * 128] = lo

    def down(i, p):
        w = wd[pl.ds(pl.multiple_of(lax.rem(i, NI) * (SB * 128), SB * 128), SB * 128)]
        y = ys.at[slot(i // NI)]
        y[...] += jnp.dot(hs[p][...], w, preferred_element_type=f32) + jnp.dot(ls[p][...], w, preferred_element_type=f32)

    norm(0)
    gates(0)
    up(0, 0)
    ys[0] = jnp.zeros((M, D), f32)

    @pl.loop(0, 4 * NI)
    def _(j):
        i = 2 * j
        for k in range(4):
            @pl.when(i == NI // 2 - 2 + 2 * ((k + 1) // 2))
            def _():
                for c in weight(k):
                    c.wait_recv()
        up(i + 1, 1)
        act(i, 0)
        down(i, 0)

        nxt = i + 2
        c = lax.rem(nxt // NI, 8)
        fresh = lax.rem(nxt, NI) == 0

        @pl.when(fresh)
        def _():
            @pl.when(c == 1)
            def _():
                for k in (0, 1):
                    for d in gather(k):
                        d.wait_recv()
                for k in (2, 3):
                    for d in gather(k):
                        d.start()

            @pl.when(c == 3)
            def _():
                for k in (2, 3):
                    for d in gather(k):
                        d.wait_recv()

            @pl.when(c == 5)
            def _():
                for k in (4, 5):
                    for d in gather(k):
                        d.wait_recv()
            norm(c)

        up(nxt, 0)
        act(i + 1, 1)
        down(i + 1, 1)

        @pl.when(fresh & (nxt < 8 * NI))
        def _():
            done = c - 1
            for k in range(4):
                @pl.when(done == 1 + k)
                def _():
                    partial(k).start()
            for k in range(2):
                @pl.when(done == 5 + k)
                def _():
                    partial(2 + k).wait_recv()
                    ys[1 + k] += rel[k]
                    partial(4 + k).start()

                @pl.when(c == 5 + k)
                def _():
                    partial(k).wait_send()

            @pl.when(c == 7)
            def _():
                partial(2).wait_send()
            ys[slot(c)] = jnp.zeros((M, D), f32)
            gates(c)

    def finish(y, a, b, x, o, dst, s):
        ca = pltpu.make_async_copy(fin.at[a], u0, lsem.at[0])
        cb = pltpu.make_async_copy(fin.at[b], u1, lsem.at[1])
        ca.start()
        cb.start()
        ca.wait()
        cb.wait()

        @pl.loop(0, M // 64)
        def _(t):
            rows = pl.ds(pl.multiple_of(t * 64, 64), 64)
            z = ys[y, rows] + u0[rows] + u1[rows]
            r = z * lax.rsqrt(jnp.mean(z * z, axis=-1, keepdims=True) + EPS) * post[...]
            xr[o, rows] = (xr[x, rows].astype(f32) + r).astype(bf16)
        co = pltpu.make_async_copy(xr.at[o], dst, lsem.at[s])
        co.start()
        return co

    partial(0).wait_recv()
    partial(1).wait_recv()
    partial(4).wait_recv()
    ob = finish(3, 1, 2, 7, 5, out.at[pl.ds(M, M)], 2)
    partial(5).wait_recv()
    oa = finish(0, 0, 3, 0, 6, out.at[pl.ds(0, M)], 3)
    for k in range(6):
        for c in gather(k):
            c.wait_send()
    for k in range(4):
        for c in weight(k):
            c.wait_send()
    for k in (3, 4, 5):
        partial(k).wait_send()
    ob.wait()
    oa.wait()


def pair_lanes(w):
    e, d, h = w.shape
    return w.reshape(e // 2, 2, d, h).transpose(0, 2, 1, 3).reshape(e // 2, d, 2 * h)


def solution(mesh):
    n = mesh.shape['wg']

    def local_block(hidden, choice, pre_scale, w_router, w_gelu, w_linear, w_down, post_scale):
        R, D = hidden.shape
        E, _, H = w_gelu.shape
        K = choice.shape[1]
        M = R // 2
        wu_own = jnp.concatenate([pair_lanes(w_gelu), pair_lanes(w_linear)], axis=-1)
        wd_own = w_down.reshape(E * H, D)
        cht = choice.reshape(2, M, K).transpose(0, 2, 1)
        any_spec = pl.BlockSpec(memory_space=pl.ANY)
        vmem = pl.BlockSpec(memory_space=pltpu.VMEM)
        sem = pltpu.SemaphoreType.DMA
        out, _ = pl.pallas_call(
            functools.partial(kernel, n),
            out_shape=[jax.ShapeDtypeStruct((R, D), bf16), jax.ShapeDtypeStruct((4, M, D), f32)],
            in_specs=[any_spec, any_spec, vmem, vmem, any_spec, any_spec, vmem],
            out_specs=[any_spec, any_spec],
            scratch_shapes=[
                pltpu.VMEM((E, D, 4 * H), bf16), pltpu.VMEM((2 * E * H, D), bf16),
                pltpu.VMEM((8, M, D), bf16), pltpu.VMEM((8, K, M), jnp.int32),
                pltpu.VMEM((M, D), bf16), pltpu.VMEM((E // 2, M, LANES), f32),
                pltpu.VMEM((M, 256 * SB), f32), pltpu.VMEM((M, 256 * SB), f32),
                pltpu.VMEM((M, 128 * SB), bf16), pltpu.VMEM((M, 128 * SB), bf16),
                pltpu.VMEM((M, 128 * SB), bf16), pltpu.VMEM((M, 128 * SB), bf16),
                pltpu.VMEM((5, M, D), f32), pltpu.VMEM((2, M, D), f32),
                sem((6,)), sem((12,)), sem((12,)), sem((8,)), sem((8,)), sem((6,)), sem((6,))],
            compiler_params=pltpu.CompilerParams(collective_id=0, has_side_effects=True, vmem_limit_bytes=67043328),
        )(hidden, cht, pre_scale.reshape(1, D), w_router, wu_own, wd_own, post_scale.reshape(1, D))
        return out

    row_spec = P(('dp', 'wg'), None)
    weight_in = P(None, None, 'wg')
    return jax.shard_map(local_block, mesh=mesh, in_specs=(row_spec, row_spec, P(), P(), weight_in, weight_in, P(None, 'wg', None), P()), out_specs=row_spec, check_vma=False)
```

```python
import functools
import jax
import jax.numpy as jnp
from jax import lax
from jax.experimental import pallas as pl
from jax.experimental.pallas import tpu as pltpu
from jax.sharding import PartitionSpec as P

EPS = 1e-5
KG = 0.7978845608028654
KC = KG * 0.044715
SB = 4
LANES = 128
f32, bf16 = jnp.float32, jnp.bfloat16


def gated_act(u, v, gate):
    w = u * (u * u * KC + KG)
    g = u * (0.5 * jnp.tanh(w) + 0.5)
    a = (g * v).astype(bf16).astype(f32)
    ga = jnp.where(gate >= 0, a * gate, 0.0)
    hi = ga.astype(bf16)
    return hi, (ga - hi.astype(f32)).astype(bf16)


def kernel(n, hid, cht, pre, wr, wg_own, wl_own, wd_own, post, out, fin,
           wu, wd, xr, chs, xb, gts, sel, u0, u1, h0, h1, l0, l1, ys, rel,
           lsem, asem, arem, vsem, wsem, wrem, ssem, srem):
    M, D = xb.shape
    Q = M // 2
    NB = wu.shape[0]
    half = NB // 2
    NI = NB // SB
    PW = half // 4
    me = lax.axis_index('wg')
    right, left = lax.rem(me + 2, n), lax.rem(me + n - 2, n)
    mate = me + 1 - 2 * lax.rem(me, 2)
    lo_h, hi_h = pl.ds(0, Q), pl.ds(Q, Q)

    barrier = pltpu.get_barrier_semaphore()
    for d in (left, right, mate):
        pl.semaphore_signal(barrier, inc=1, device_id={'wg': d}, device_id_type=pl.DeviceIdType.MESH)
    pl.semaphore_wait(barrier, 3)

    def remote(src, dst, ss, rs, dev):
        return pltpu.make_async_remote_copy(src_ref=src, dst_ref=dst, send_sem=ss, recv_sem=rs,
                                            device_id={'wg': dev}, device_id_type=pl.DeviceIdType.MESH)

    def gather(k, side):
        dev, land, own = ((right, lo_h, (0, 1, 2, 3)), (left, hi_h, (2, 3, 0, 1)))[side]
        if k < 4:
            q = own[k]
            c = (1, 2, 5, 6)[k]
            x_src, c_src, at = hid.at[pl.ds(q * Q, Q)], cht.at[:, pl.ds(q * Q, Q)], land
        else:
            c = k - 1
            x_src, c_src, at = xr.at[k - 3, land], chs.at[k - 3, :, land], (hi_h, lo_h)[side]
        s = 12 * side + 2 * k
        return (remote(c_src, chs.at[c, :, at], asem.at[s], arem.at[s], dev),
                remote(x_src, xr.at[c, at], asem.at[s + 1], arem.at[s + 1], dev))

    def pieces(k, base):
        b, w = pl.ds(base + k * PW, PW), pl.ds((base + k * PW) * LANES, PW * LANES)
        s, v = pl.ds(k * PW, PW), pl.ds(k * PW * LANES, PW * LANES)
        return ((wg_own.at[s], wu.at[b, pl.ds(0, LANES)]), (wl_own.at[s], wu.at[b, pl.ds(LANES, LANES)]),
                (wd_own.at[v], wd.at[w]))

    def weight(k):
        return [remote(src, dst, wsem.at[3 * k + t], wrem.at[3 * k + t], mate)
                for t, (src, dst) in enumerate(pieces(k, half))]

    def load(k):
        return [pltpu.make_async_copy(src, dst, vsem.at[3 * k + t]) for t, (src, dst) in enumerate(pieces(k, 0))]

    def partial(c, side):
        dev, at = ((left, lo_h), (right, hi_h))[side]
        s = c - 4 * (c // 5)
        to = (lo_h, hi_h)[(c - 1) % 2]
        if c < 3:
            dst = fin.at[side, to]
        elif c < 5:
            dst = rel.at[c - 3, at]
        else:
            dst = fin.at[3 - side, to]
        k = 2 * (c - 1) + side
        return remote(ys.at[s, at], dst, ssem.at[k], srem.at[k], dev)

    SIDES = (0, 1)
    for k in range(4):
        for side in SIDES:
            for d in gather(k, side):
                d.start()
    local = [pltpu.make_async_copy(hid.at[pl.ds(0, M)], xr.at[0], lsem.at[0]),
             pltpu.make_async_copy(cht.at[:, pl.ds(0, M)], chs.at[0], lsem.at[1]),
             pltpu.make_async_copy(hid.at[pl.ds(M, M)], xr.at[7], lsem.at[2]),
             pltpu.make_async_copy(cht.at[:, pl.ds(M, M)], chs.at[7], lsem.at[3])]
    for d in local:
        d.start()
    for k in range(4):
        for d in load(k):
            d.start()
    for k in range(4):
        for d in weight(k):
            d.start()
    for d in local:
        d.wait()

    us, hs, ls = (u0, u1), (h0, h1), (l0, l1)
    nt = (((1,), (1,)), ((), ()))

    def norm(c):
        for t in range(2):
            rows = pl.ds(t * Q, Q)
            x = xr[c, rows].astype(f32)
            xb[rows] = (x * lax.rsqrt(jnp.mean(x * x, axis=-1, keepdims=True) + EPS) * pre[...]).astype(bf16)

    E = wr.shape[0]
    iota = lax.broadcasted_iota
    expert_row = lax.rem(iota(jnp.int32, (3 * E, LANES), 0), E)
    for q in range(E // 2):
        lane = iota(jnp.int32, (3 * E, LANES), 1)
        sel[:, q * LANES:(q + 1) * LANES] = jnp.where(expert_row == 2 * q + lane // (LANES // 2), 1.0, 0.0).astype(bf16)

    def gates(c):
        w3 = jnp.concatenate([wr[...]] * 3, axis=0)
        logits = lax.dot_general(xb[...], w3, nt, preferred_element_type=f32)
        lane = iota(jnp.int32, (M, 3 * E), 1)
        e = jnp.exp(logits - logits.max(-1, keepdims=True))
        p = e / jnp.where(lane < E, e, 0.0).sum(-1, keepdims=True)
        ch = chs[c]
        ids = iota(jnp.int32, (E, M), 0)
        hit = ch[0:1] == ids
        for j in range(1, ch.shape[0]):
            hit = hit | (ch[j:j + 1] == ids)
        eye3 = jnp.where(iota(jnp.int32, (E, 3 * E), 0) == lax.rem(iota(jnp.int32, (E, 3 * E), 1), E), 1.0, 0.0)
        mask = lax.dot_general(jnp.where(hit, 1.0, 0.0).astype(bf16), eye3.astype(bf16), (((0,), (0,)), ((), ())),
                               preferred_element_type=f32)
        g = jnp.where(mask > 0.5, p, -1.0)
        top = g.astype(bf16).astype(f32)
        mid = (g - top).astype(bf16).astype(f32)
        g3 = jnp.where(lane < E, top, jnp.where(lane < 2 * E, mid, g - top - mid)).astype(bf16)
        for q in range(0, E // 2, 2):
            t = jnp.dot(g3, sel[:, q * LANES:(q + 2) * LANES], preferred_element_type=f32)
            gts[q] = t[:, :LANES]
            gts[q + 1] = t[:, LANES:]

    def slot(c):
        return c - 4 * (c // 5)

    def up(i, p, ks=range(SB)):
        b = lax.rem(i, NI) * SB
        for k in ks:
            us[p][:, k * 256:(k + 1) * 256] = lax.dot_general(xb[...], wu[b + k], nt, preferred_element_type=f32)

    def act(i, p, ks):
        b = lax.rem(i * SB, half)
        for k in ks:
            hi, lo = gated_act(us[p][:, k * 256:k * 256 + 128], us[p][:, k * 256 + 128:(k + 1) * 256], gts[b + k])
            hs[p][:, k * 128:(k + 1) * 128] = hi
            ls[p][:, k * 128:(k + 1) * 128] = lo

    def down(i, p):
        w = wd[pl.ds(pl.multiple_of(lax.rem(i, NI) * (SB * 128), SB * 128), SB * 128)]
        y = ys.at[slot(i // NI)]
        y[...] += jnp.dot(hs[p][...], w, preferred_element_type=f32) + jnp.dot(ls[p][...], w, preferred_element_type=f32)

    def step(i, p):
        for k in range(SB):
            up(i + 1, 1 - p, (k,))
            act(i, p, (k,))
        down(i, p)

    norm(0)
    gates(0)
    for d in load(0):
        d.wait()
    up(0, 0)
    ys[0] = jnp.zeros((M, D), f32)

    @pl.loop(0, 4 * NI)
    def _(j):
        i = 2 * j

        @pl.when(i == 0)
        def _():
            for k in range(1, 4):
                for d in load(k):
                    d.wait()
        for k in range(4):
            @pl.when(i == NI // 2 - 2 + 2 * ((k + 1) // 2))
            def _():
                for d in weight(k):
                    d.wait_recv()
        step(i, 0)

        nxt = i + 2
        c = lax.rem(nxt // NI, 8)
        fresh = lax.rem(nxt, NI) == 0

        @pl.when(fresh)
        def _():
            for a in range(6):
                @pl.when(c == 1 + a)
                def _():
                    k = (0, 1, 4, 5, 2, 3)[a]
                    for side in SIDES:
                        for d in gather(k, side):
                            d.wait_recv()
                    if k < 2:
                        for side in SIDES:
                            for d in gather(k + 4, side):
                                d.start()
            norm(c)

        step(i + 1, 1)

        @pl.when(fresh & (nxt < 8 * NI))
        def _():
            for a in range(1, 7):
                @pl.when(c - 1 == a)
                def _():
                    if a > 4:
                        for side in SIDES:
                            partial(a - 2, side).wait_recv()
                        ys[a - 4] += rel[a - 5]
                    for side in SIDES:
                        partial(a, side).start()
                if a < 4:
                    @pl.when(c == a + 4)
                    def _():
                        for side in SIDES:
                            partial(a, side).wait_send()
            ys[slot(c)] = jnp.zeros((M, D), f32)
            gates(c)

    def finish(q, p):
        early, late = (0, 2) if q < 2 else (1, 3)
        rows_q = pl.ds((q % 2) * Q, Q)
        buf = us[p]
        ca = pltpu.make_async_copy(fin.at[early, rows_q], buf.at[lo_h], lsem.at[0])
        cb = pltpu.make_async_copy(fin.at[late, rows_q], buf.at[hi_h], lsem.at[1])
        ca.start()
        cb.start()
        ca.wait()
        cb.wait()
        y, x = ((0, 0), (3, 7))[q // 2]
        r0 = (q % 2) * Q

        @pl.loop(0, Q // 64)
        def _(t):
            rows = pl.ds(pl.multiple_of(r0 + t * 64, 64), 64)
            z = ys[y, rows] + buf[pl.ds(pl.multiple_of(t * 64, 64), 64)] + buf[pl.ds(pl.multiple_of(Q + t * 64, 64), 64)]
            r = z * lax.rsqrt(jnp.mean(z * z, axis=-1, keepdims=True) + EPS) * post[...]
            xr[5 + q // 2, rows] = (xr[x, rows].astype(f32) + r).astype(bf16)
        co = pltpu.make_async_copy(xr.at[5 + q // 2, rows_q], out.at[pl.ds(q * Q, Q)], vsem.at[q])
        co.start()
        return co

    for c in (1, 2):
        for side in SIDES:
            partial(c, side).wait_recv()
    for side in SIDES:
        partial(5, side).wait_recv()
    done = [finish(0, 0), finish(2, 1)]
    for side in SIDES:
        partial(6, side).wait_recv()
    done += [finish(1, 0), finish(3, 1)]
    for k in range(6):
        for side in SIDES:
            for d in gather(k, side):
                d.wait_send()
    for k in range(4):
        for d in weight(k):
            d.wait_send()
    for c in (4, 5, 6):
        for side in SIDES:
            partial(c, side).wait_send()
    for d in done:
        d.wait()


def pairs(w):
    e, d, h = w.shape
    return w.transpose(0, 2, 1).reshape(e // 2, 2 * h, d)


def solution(mesh):
    n = mesh.shape['wg']

    def local_block(hidden, choice, pre_scale, w_router, w_gelu, w_linear, w_down, post_scale):
        R, D = hidden.shape
        E, _, H = w_gelu.shape
        K = choice.shape[1]
        M = R // 2
        wd_own = w_down.reshape(E * H, D)
        cht = choice.T
        any_spec = pl.BlockSpec(memory_space=pl.ANY)
        vmem = pl.BlockSpec(memory_space=pltpu.VMEM)
        sem = pltpu.SemaphoreType.DMA
        out, _ = pl.pallas_call(
            functools.partial(kernel, n),
            out_shape=[jax.ShapeDtypeStruct((R, D), bf16), jax.ShapeDtypeStruct((4, M, D), f32)],
            in_specs=[any_spec, any_spec, vmem, vmem, any_spec, any_spec, any_spec, vmem],
            out_specs=[any_spec, any_spec],
            scratch_shapes=[
                pltpu.VMEM((E, 4 * H, D), bf16), pltpu.VMEM((2 * E * H, D), bf16),
                pltpu.VMEM((8, M, D), bf16), pltpu.VMEM((8, K, M), jnp.int32),
                pltpu.VMEM((M, D), bf16), pltpu.VMEM((E // 2, M, LANES), f32), pltpu.VMEM((3 * E, E // 2 * LANES), bf16),
                pltpu.VMEM((M, 256 * SB), f32), pltpu.VMEM((M, 256 * SB), f32),
                pltpu.VMEM((M, 128 * SB), bf16), pltpu.VMEM((M, 128 * SB), bf16),
                pltpu.VMEM((M, 128 * SB), bf16), pltpu.VMEM((M, 128 * SB), bf16),
                pltpu.VMEM((5, M, D), f32), pltpu.VMEM((2, M, D), f32),
                sem((4,)), sem((24,)), sem((24,)), sem((12,)), sem((12,)), sem((12,)), sem((12,)), sem((12,))],
            compiler_params=pltpu.CompilerParams(collective_id=0, has_side_effects=True, vmem_limit_bytes=67043328),
        )(hidden, cht, pre_scale.reshape(1, D), w_router.T, pairs(w_gelu), pairs(w_linear), wd_own, post_scale.reshape(1, D))
        return out

    row_spec = P(('dp', 'wg'), None)
    weight_in = P(None, None, 'wg')
    return jax.shard_map(local_block, mesh=mesh, in_specs=(row_spec, row_spec, P(), P(), weight_in, weight_in, P(None, 'wg', None), P()), out_specs=row_spec, check_vma=False)
```

```python
import functools
import jax
import jax.numpy as jnp
from jax import lax
from jax.experimental import pallas as pl
from jax.experimental.pallas import tpu as pltpu
from jax.sharding import PartitionSpec as P

EPS = 1e-5
KG = 0.7978845608028654
KC = KG * 0.044715
SB = 4
LANES = 128
f32, bf16 = jnp.float32, jnp.bfloat16


def gated_act(u, v, gate):
    w = u * (u * u * KC + KG)
    g = u * (0.5 * jnp.tanh(w) + 0.5)
    a = (g * v).astype(bf16).astype(f32)
    ga = jnp.where(gate >= 0, a * gate, 0.0)
    hi = ga.astype(bf16)
    return hi, (ga - hi.astype(f32)).astype(bf16)


def kernel(n, hid, cht, pre, wr, wg_own, wl_own, wd_own, post, out, fin,
           wu, wd, xr, chs, g3, sel, u0, u1, h0, h1, l0, l1, ys, rel, lat,
           lsem, asem, arem, vsem, wsem, wrem, ssem, srem, osem):
    M, D = xr.shape[1:]
    Q = M // 2
    pairs_n = wu.shape[0]
    PS = SB // 2
    NI = pairs_n // PS
    me = lax.axis_index('wg')
    right, left = lax.rem(me + 2, n), lax.rem(me + n - 2, n)
    mate = me + 1 - 2 * lax.rem(me, 2)
    lo_h, hi_h = pl.ds(0, Q), pl.ds(Q, Q)

    barrier = pltpu.get_barrier_semaphore()
    for d in (left, right, mate):
        pl.semaphore_signal(barrier, inc=1, device_id={'wg': d}, device_id_type=pl.DeviceIdType.MESH)
    pl.semaphore_wait(barrier, 3)

    def remote(src, dst, ss, rs, dev):
        return pltpu.make_async_remote_copy(src_ref=src, dst_ref=dst, send_sem=ss, recv_sem=rs,
                                            device_id={'wg': dev}, device_id_type=pl.DeviceIdType.MESH)

    def gather(k, side):
        dev, land, own = ((right, lo_h, (0, 1, 2, 3)), (left, hi_h, (2, 3, 0, 1)))[side]
        if k < 4:
            q = own[k]
            c = (1, 2, 5, 6)[k]
            x_src, c_src, at = hid.at[pl.ds(q * Q, Q)], cht.at[:, pl.ds(q * Q, Q)], land
        else:
            c = k - 1
            x_src, c_src, at = xr.at[k - 3, land], chs.at[k - 3, :, land], (hi_h, lo_h)[side]
        s = 12 * side + 2 * k
        return (remote(c_src, chs.at[c, :, at], asem.at[s], arem.at[s], dev),
                remote(x_src, xr.at[c, at], asem.at[s + 1], arem.at[s + 1], dev))

    def pieces(k, h):
        p = pl.ds(k * PS, PS)
        return ((wg_own.at[p], wu.at[p, h, pl.ds(0, LANES)]), (wl_own.at[p], wu.at[p, h, pl.ds(LANES, LANES)]),
                (wd_own.at[p], wd.at[p, h]))

    def weight(k):
        return [remote(src, dst, wsem.at[3 * k + t], wrem.at[3 * k + t], mate)
                for t, (src, dst) in enumerate(pieces(k, 1))]

    def load(k):
        return [pltpu.make_async_copy(src, dst, vsem.at[3 * k + t]) for t, (src, dst) in enumerate(pieces(k, 0))]

    def arrived(k):
        for d in load(k):
            d.wait()
        for d in weight(k):
            d.wait_recv()

    def partial(c, side, h=0):
        dev, base = ((left, 0), (right, Q))[side]
        s = c - 4 * (c // 5)
        to = ((c - 1) % 2) * Q
        if c < 5:
            at = pl.ds(base, Q)
            dst = fin.at[side, pl.ds(to, Q)] if c < 3 else rel.at[c - 3, at]
        else:
            at = pl.ds(base + h * (Q // 2), Q // 2)
            dst = lat.at[1 - side, pl.ds(to + h * (Q // 2), Q // 2)]
        k = 4 * (c - 1) + 2 * side + h
        return remote(ys.at[s, at], dst, ssem.at[k], srem.at[k], dev)

    SIDES = (0, 1)
    for k in range(4):
        for side in SIDES:
            for d in gather(k, side):
                d.start()
    local = [pltpu.make_async_copy(hid.at[pl.ds(0, M)], xr.at[0], lsem.at[0]),
             pltpu.make_async_copy(cht.at[:, pl.ds(0, M)], chs.at[0], lsem.at[1]),
             pltpu.make_async_copy(hid.at[pl.ds(M, M)], xr.at[7], lsem.at[2]),
             pltpu.make_async_copy(cht.at[:, pl.ds(M, M)], chs.at[7], lsem.at[3])]
    for d in local:
        d.start()
    for k in range(NI):
        for d in load(k) + weight(k):
            d.start()
    E = wr.shape[0]
    iota = lax.broadcasted_iota
    expert_row = lax.rem(iota(jnp.int32, (3 * E, LANES), 0), E)
    for q in range(E // 2):
        lane = iota(jnp.int32, (3 * E, LANES), 1)
        sel[q // PS, :, (q % PS) * LANES:(q % PS + 1) * LANES] = jnp.where(
            expert_row == 2 * q + lane // (LANES // 2), 1.0, 0.0).astype(bf16)

    for d in local:
        d.wait()

    again = [pltpu.make_async_copy(hid.at[pl.ds(k * M, M)], xr.at[1 + k], lsem.at[2 * k]) for k in range(2)]
    us, hs, ls = (u0, u1), (h0, h1), (l0, l1)
    nt = (((1,), (1,)), ((), ()))

    def norm(c):
        for t in range(2):
            rows = pl.ds(t * Q, Q)
            x = xr[c, rows].astype(f32)
            xr[c, rows] = (x * lax.rsqrt(jnp.mean(x * x, axis=-1, keepdims=True) + EPS) * pre[...]).astype(bf16)

    def gates(c):
        w3 = jnp.concatenate([wr[...]] * 3, axis=0)
        logits = lax.dot_general(xr[c], w3, nt, preferred_element_type=f32)
        lane = iota(jnp.int32, (M, 3 * E), 1)
        e = jnp.exp(logits - logits.max(-1, keepdims=True))
        p = e / jnp.where(lane < E, e, 0.0).sum(-1, keepdims=True)
        ch = chs[c]
        ids = iota(jnp.int32, (E, M), 0)
        hit = ch[0:1] == ids
        for j in range(1, ch.shape[0]):
            hit = hit | (ch[j:j + 1] == ids)
        eye3 = jnp.where(iota(jnp.int32, (E, 3 * E), 0) == lax.rem(iota(jnp.int32, (E, 3 * E), 1), E), 1.0, 0.0)
        mask = lax.dot_general(jnp.where(hit, 1.0, 0.0).astype(bf16), eye3.astype(bf16), (((0,), (0,)), ((), ())),
                               preferred_element_type=f32)
        g = jnp.where(mask > 0.5, p, -1.0)
        top = g.astype(bf16).astype(f32)
        mid = (g - top).astype(bf16).astype(f32)
        g3[...] = jnp.where(lane < E, top, jnp.where(lane < 2 * E, mid, g - top - mid)).astype(bf16)

    def slot(c):
        return c - 4 * (c // 5)

    def up(i, p, ks):
        b = lax.rem(i, NI) * PS
        x = xr.at[lax.rem(i // NI, 8)]
        for k in ks:
            us[p][:, k * 256:(k + 1) * 256] = lax.dot_general(x[...], wu[b + k // 2, k % 2], nt, preferred_element_type=f32)

    def act(p, ks, gate):
        for k in ks:
            hi, lo = gated_act(us[p][:, k * 256:k * 256 + 128], us[p][:, k * 256 + 128:(k + 1) * 256],
                               gate[:, (k // 2) * LANES:(k // 2 + 1) * LANES])
            hs[p][:, k * 128:(k + 1) * 128] = hi
            ls[p][:, k * 128:(k + 1) * 128] = lo

    def down(i, p, t):
        r = PS * LANES
        w = wd[pl.ds(lax.rem(i, NI) * PS + t * (PS // 2), PS // 2)].reshape(r, D)
        y = ys.at[slot(i // NI)]
        cols = pl.ds(t * r, r)
        old = y[...]
        if t == 0:
            old = jnp.where(lax.rem(i, NI) == 0, 0.0, old)
        y[...] = old + (jnp.dot(hs[p][:, cols], w, preferred_element_type=f32) + jnp.dot(ls[p][:, cols], w, preferred_element_type=f32))

    def step(i, p):
        gate = jnp.dot(g3[...], sel[lax.rem(i, NI)], preferred_element_type=f32)
        act(p, range(SB // 2), gate)
        up(i + 1, 1 - p, range(SB // 2))
        act(p, range(SB // 2, SB), gate)
        down(i, p, 0)
        up(i + 1, 1 - p, range(SB // 2, SB))
        down(i, p, 1)

    norm(0)
    gates(0)
    arrived(0)
    up(0, 0, range(SB))

    @pl.loop(0, 4 * NI)
    def _(j):
        i = 2 * j

        for k in range(1, NI, 2):
            @pl.when(i == k - 1)
            def _():
                arrived(k)
        step(i, 0)

        nxt = i + 2
        for k in range(2, NI, 2):
            @pl.when(nxt == k)
            def _():
                arrived(k)
        c = lax.rem(nxt // NI, 8)
        fresh = lax.rem(nxt, NI) == 0

        @pl.when(fresh)
        def _():
            for a in range(6):
                @pl.when(c == 1 + a)
                def _():
                    for side in SIDES:
                        for d in gather((0, 1, 4, 5, 2, 3)[a], side):
                            d.wait_recv()

            @pl.when((c != 3) & (c != 4))
            def _():
                norm(c)
            for a in range(2):
                @pl.when(c == 1 + a)
                def _():
                    for side in SIDES:
                        for d in gather(a + 4, side):
                            d.start()

            @pl.when(c == 5)
            def _():
                for k in (4, 5):
                    for side in SIDES:
                        for d in gather(k, side):
                            d.wait_send()
                for d in again:
                    d.start()

        step(i + 1, 1)

        @pl.when(fresh & (nxt < 8 * NI))
        def _():
            for a in range(1, 7):
                @pl.when(c - 1 == a)
                def _():
                    if a > 4:
                        for side in SIDES:
                            partial(a - 2, side).wait_recv()
                        ys[a - 4] += rel[a - 5]
                    for h in range(1 + a // 5):
                        for side in SIDES:
                            partial(a, side, h).start()
                if a < 4:
                    @pl.when(c == a + 4)
                    def _():
                        for side in SIDES:
                            partial(a, side).wait_send()
            gates(c)

    BLK = Q // 2
    staged = {}

    def stage(t, dst, src, k):
        d = pltpu.make_async_copy(src, dst, vsem.at[k])
        d.start()
        staged[t] = d

    def early(q):
        return fin.at[q // 2, pl.ds((q % 2) * Q, Q)]

    def home(q):
        return (0, 3)[q // 2], 1 + q // 2, (q % 2) * Q

    def finish(q, h):
        y, x, r0 = home(q)
        rows = pl.ds(r0 + h * BLK, BLK)
        z = ys[y, rows] + lat[q // 2, rows]
        r = z * lax.rsqrt(jnp.mean(z * z, axis=-1, keepdims=True) + EPS) * post[...]
        xr[5 + q // 2, rows] = (xr[x, rows].astype(f32) + r).astype(bf16)
        co = pltpu.make_async_copy(xr.at[5 + q // 2, rows], out.at[pl.ds(q * Q + h * BLK, BLK)], osem.at[2 * q + h])
        co.start()
        return co

    for c in (1, 2):
        for side in SIDES:
            partial(c, side).wait_recv()
    bufs = {0: u0.at[lo_h, pl.ds(0, D)], 2: u0.at[hi_h, pl.ds(0, D)], 1: u1.at[lo_h, pl.ds(0, D)], 3: u1.at[hi_h, pl.ds(0, D)]}
    for q in range(4):
        stage(q, bufs[q], early(q), q)
    for q in range(4):
        staged[q].wait()
        y, x, r0 = home(q)
        ys[y, pl.ds(r0, Q)] += bufs[q][...]
    for d in again:
        d.wait()
    done = []
    for half_q, c in ((0, 5), (1, 6)):
        for h in range(2):
            for side in SIDES:
                partial(c, side, h).wait_recv()
            for q in (half_q, half_q + 2):
                done.append(finish(q, h))
    for k in range(4):
        for side in SIDES:
            for d in gather(k, side):
                d.wait_send()
    for k in range(NI):
        for d in weight(k):
            d.wait_send()
    for c in (4, 5, 6):
        for h in range(1 + c // 5):
            for side in SIDES:
                partial(c, side, h).wait_send()
    for d in done:
        d.wait()


def pairs(w):
    e, d, h = w.shape
    return w.transpose(0, 2, 1).reshape(e // 2, 2 * h, d)


def solution(mesh):
    n = mesh.shape['wg']

    def local_block(hidden, choice, pre_scale, w_router, w_gelu, w_linear, w_down, post_scale):
        R, D = hidden.shape
        E, _, H = w_gelu.shape
        K = choice.shape[1]
        M = R // 2
        wd_own = w_down.reshape(E // 2, 2 * H, D)
        cht = choice.T
        any_spec = pl.BlockSpec(memory_space=pl.ANY)
        vmem = pl.BlockSpec(memory_space=pltpu.VMEM)
        sem = pltpu.SemaphoreType.DMA
        out, _ = pl.pallas_call(
            functools.partial(kernel, n),
            out_shape=[jax.ShapeDtypeStruct((R, D), bf16), jax.ShapeDtypeStruct((2, M, D), f32)],
            in_specs=[any_spec, any_spec, vmem, vmem, any_spec, any_spec, any_spec, vmem],
            out_specs=[any_spec, any_spec],
            scratch_shapes=[
                pltpu.VMEM((E // 2, 2, 4 * H, D), bf16), pltpu.VMEM((E // 2, 2, 2 * H, D), bf16),
                pltpu.VMEM((8, M, D), bf16), pltpu.VMEM((8, K, M), jnp.int32),
                pltpu.VMEM((M, 3 * E), bf16), pltpu.VMEM((E // SB, 3 * E, SB // 2 * LANES), bf16),
                pltpu.VMEM((M, 256 * SB), f32), pltpu.VMEM((M, 256 * SB), f32),
                pltpu.VMEM((M, 128 * SB), bf16), pltpu.VMEM((M, 128 * SB), bf16),
                pltpu.VMEM((M, 128 * SB), bf16), pltpu.VMEM((M, 128 * SB), bf16),
                pltpu.VMEM((5, M, D), f32), pltpu.VMEM((2, M, D), f32), pltpu.VMEM((2, M, D), f32),
                sem((4,)), sem((24,)), sem((24,)), sem((3 * E // SB,)), sem((3 * E // SB,)), sem((3 * E // SB,)), sem((24,)), sem((24,)), sem((8,))],
            compiler_params=pltpu.CompilerParams(collective_id=0, has_side_effects=True, vmem_limit_bytes=67043328),
        )(hidden, cht, pre_scale.reshape(1, D), w_router.T, pairs(w_gelu), pairs(w_linear), wd_own, post_scale.reshape(1, D))
        return out

    row_spec = P(('dp', 'wg'), None)
    weight_in = P(None, None, 'wg')
    return jax.shard_map(local_block, mesh=mesh, in_specs=(row_spec, row_spec, P(), P(), weight_in, weight_in, P(None, 'wg', None), P()), out_specs=row_spec, check_vma=False)
```

```python
import functools
import jax
import jax.numpy as jnp
from jax import lax
from jax.experimental import pallas as pl
from jax.experimental.pallas import tpu as pltpu
from jax.sharding import PartitionSpec as P

EPS = 1e-5
KG = 0.7978845608028654
KC = KG * 0.044715
SB = 4
LANES = 128
f32, bf16 = jnp.float32, jnp.bfloat16


def gated_act(u, v, gate):
    w = u * (u * u * KC + KG)
    g = u * (0.5 * jnp.tanh(w) + 0.5)
    a = (g * v).astype(bf16).astype(f32)
    ga = jnp.where(gate >= 0, a * gate, 0.0)
    hi = ga.astype(bf16)
    return hi, (ga - hi.astype(f32)).astype(bf16)


def kernel(n, hid, cht, pre, wr, wg_own, wl_own, wd_own, post, out, fin,
           wu, wd, xr, chs, g3, sel, u0, u1, h0, h1, l0, l1, ys, rel, lat,
           lsem, asem, arem, vsem, wsem, wrem, ssem, srem, osem):
    M, D = xr.shape[1:]
    Q = M // 2
    pairs_n = wu.shape[0]
    PS = SB // 2
    NI = pairs_n // PS
    me = lax.axis_index('wg')
    right, left = lax.rem(me + 2, n), lax.rem(me + n - 2, n)
    mate = me + 1 - 2 * lax.rem(me, 2)
    lo_h, hi_h = pl.ds(0, Q), pl.ds(Q, Q)

    barrier = pltpu.get_barrier_semaphore()
    for d in (left, right, mate):
        pl.semaphore_signal(barrier, inc=1, device_id={'wg': d}, device_id_type=pl.DeviceIdType.MESH)
    pl.semaphore_wait(barrier, 3)

    def remote(src, dst, ss, rs, dev):
        return pltpu.make_async_remote_copy(src_ref=src, dst_ref=dst, send_sem=ss, recv_sem=rs,
                                            device_id={'wg': dev}, device_id_type=pl.DeviceIdType.MESH)

    def gather_at(k, side):
        dev, land, own = ((right, lo_h, (0, 1, 2, 3)), (left, hi_h, (2, 3, 0, 1)))[side]
        if k < 4:
            q = own[k]
            c = (1, 2, 5, 6)[k]
            x_src, c_src, at = hid.at[pl.ds(q * Q, Q)], chs.at[(0, 7)[q // 2], :, pl.ds((q % 2) * Q, Q)], land
        else:
            c = k - 1
            x_src, c_src, at = xr.at[k - 3, land], chs.at[k - 3, :, land], (hi_h, lo_h)[side]
        s = 12 * side + 2 * k
        return c_src, x_src, c, at, s, dev

    def gather_ids(k, side):
        c_src, _, c, at, s, dev = gather_at(k, side)
        return remote(c_src, chs.at[c, :, at], asem.at[s], arem.at[s], dev)

    def gather_rows(k, side):
        _, x_src, c, at, s, dev = gather_at(k, side)
        return remote(x_src, xr.at[c, at], asem.at[s + 1], arem.at[s + 1], dev)

    def gather(k, side):
        return gather_ids(k, side), gather_rows(k, side)

    def pieces(k, h):
        p = pl.ds(k * PS, PS)
        return ((wg_own.at[p], wu.at[p, h, pl.ds(0, LANES)]), (wl_own.at[p], wu.at[p, h, pl.ds(LANES, LANES)]),
                (wd_own.at[p], wd.at[p, h]))

    def weight(k):
        return [remote(src, dst, wsem.at[3 * k + t], wrem.at[3 * k + t], mate)
                for t, (src, dst) in enumerate(pieces(k, 1))]

    def load(k):
        return [pltpu.make_async_copy(src, dst, vsem.at[3 * k + t]) for t, (src, dst) in enumerate(pieces(k, 0))]

    def arrived(k):
        for d in load(k):
            d.wait()
        for d in weight(k):
            d.wait_recv()

    def partial(c, side, h=0):
        dev, base = ((left, 0), (right, Q))[side]
        s = c - 4 * (c // 5)
        to = ((c - 1) % 2) * Q
        if c < 5:
            at = pl.ds(base, Q)
            dst = fin.at[side, pl.ds(to, Q)] if c < 3 else rel.at[c - 3, at]
        else:
            at = pl.ds(base + h * (Q // 2), Q // 2)
            dst = lat.at[1 - side, pl.ds(to + h * (Q // 2), Q // 2)]
        k = 4 * (c - 1) + 2 * side + h
        return remote(ys.at[s, at], dst, ssem.at[k], srem.at[k], dev)

    SIDES = (0, 1)
    for side in SIDES:
        gather_rows(0, side).start()
    chs[0] = cht[:, :M].astype(f32).astype(bf16)
    chs[7] = cht[:, M:].astype(f32).astype(bf16)
    local = [pltpu.make_async_copy(hid.at[pl.ds(0, M)], xr.at[0], lsem.at[0]),
             pltpu.make_async_copy(hid.at[pl.ds(M, M)], xr.at[7], lsem.at[2])]
    for d in local:
        d.start()
    for k in range(NI):
        for d in load(k) + weight(k):
            d.start()
    for k in range(4):
        for side in SIDES:
            gather_ids(k, side).start()
            if k:
                gather_rows(k, side).start()
    E = wr.shape[0]
    iota = lax.broadcasted_iota
    expert_row = lax.rem(iota(jnp.int32, (3 * E, LANES), 0), E)
    for q in range(E // 2):
        lane = iota(jnp.int32, (3 * E, LANES), 1)
        sel[q // PS, :, (q % PS) * LANES:(q % PS + 1) * LANES] = jnp.where(
            expert_row == 2 * q + lane // (LANES // 2), 1.0, 0.0).astype(bf16)

    for d in local:
        d.wait()

    again = [pltpu.make_async_copy(hid.at[pl.ds(k * M, M)], xr.at[1 + k], lsem.at[2 * k]) for k in range(2)]
    us, hs, ls = (u0, u1), (h0, h1), (l0, l1)
    nt = (((1,), (1,)), ((), ()))

    def norm(c):
        for t in range(2):
            rows = pl.ds(t * Q, Q)
            x = xr[c, rows].astype(f32)
            xr[c, rows] = (x * lax.rsqrt(jnp.mean(x * x, axis=-1, keepdims=True) + EPS) * pre[...]).astype(bf16)

    def gates(c):
        w3 = jnp.concatenate([wr[...]] * 3, axis=0)
        logits = lax.dot_general(xr[c], w3, nt, preferred_element_type=f32)
        lane = iota(jnp.int32, (M, 3 * E), 1)
        e = jnp.exp(logits - logits.max(-1, keepdims=True))
        p = e / jnp.where(lane < E, e, 0.0).sum(-1, keepdims=True)
        ch = chs[c].astype(f32)
        ids = iota(jnp.int32, (E, M), 0).astype(f32)
        hit = ch[0:1] == ids
        for j in range(1, ch.shape[0]):
            hit = hit | (ch[j:j + 1] == ids)
        eye3 = jnp.where(iota(jnp.int32, (E, 3 * E), 0) == lax.rem(iota(jnp.int32, (E, 3 * E), 1), E), 1.0, 0.0)
        mask = lax.dot_general(jnp.where(hit, 1.0, 0.0).astype(bf16), eye3.astype(bf16), (((0,), (0,)), ((), ())),
                               preferred_element_type=f32)
        g = jnp.where(mask > 0.5, p, -1.0)
        top = g.astype(bf16).astype(f32)
        mid = (g - top).astype(bf16).astype(f32)
        g3[...] = jnp.where(lane < E, top, jnp.where(lane < 2 * E, mid, g - top - mid)).astype(bf16)

    def slot(c):
        return c - 4 * (c // 5)

    def up(i, p, ks):
        b = lax.rem(i, NI) * PS
        x = xr.at[lax.rem(i // NI, 8)]
        for k in ks:
            us[p][:, k * 256:(k + 1) * 256] = lax.dot_general(x[...], wu[b + k // 2, k % 2], nt, preferred_element_type=f32)

    def act(p, ks, gate):
        for k in ks:
            hi, lo = gated_act(us[p][:, k * 256:k * 256 + 128], us[p][:, k * 256 + 128:(k + 1) * 256],
                               gate[:, (k // 2) * LANES:(k // 2 + 1) * LANES])
            hs[p][:, k * 128:(k + 1) * 128] = hi
            ls[p][:, k * 128:(k + 1) * 128] = lo

    def down(i, p, t):
        r = PS * LANES
        w = wd[pl.ds(lax.rem(i, NI) * PS + t * (PS // 2), PS // 2)].reshape(r, D)
        y = ys.at[slot(i // NI)]
        cols = pl.ds(t * r, r)
        old = y[...]
        if t == 0:
            old = jnp.where(lax.rem(i, NI) == 0, 0.0, old)
        y[...] = old + (jnp.dot(hs[p][:, cols], w, preferred_element_type=f32) + jnp.dot(ls[p][:, cols], w, preferred_element_type=f32))

    def step(i, p):
        gate = jnp.dot(g3[...], sel[lax.rem(i, NI)], preferred_element_type=f32)
        act(p, range(SB // 2), gate)
        up(i + 1, 1 - p, range(SB // 2))
        act(p, range(SB // 2, SB), gate)
        down(i, p, 0)
        up(i + 1, 1 - p, range(SB // 2, SB))
        down(i, p, 1)

    norm(0)
    gates(0)
    arrived(0)
    up(0, 0, range(SB))

    @pl.loop(0, 4 * NI)
    def _(j):
        i = 2 * j

        for k in range(1, NI, 2):
            @pl.when(i == k - 1)
            def _():
                arrived(k)
        step(i, 0)

        nxt = i + 2
        for k in range(2, NI, 2):
            @pl.when(nxt == k)
            def _():
                arrived(k)
        c = lax.rem(nxt // NI, 8)
        fresh = lax.rem(nxt, NI) == 0

        @pl.when(fresh)
        def _():
            for a in range(6):
                @pl.when(c == 1 + a)
                def _():
                    for side in SIDES:
                        for d in gather((0, 1, 4, 5, 2, 3)[a], side):
                            d.wait_recv()

            @pl.when((c != 3) & (c != 4))
            def _():
                norm(c)
            for a in range(2):
                @pl.when(c == 1 + a)
                def _():
                    for side in SIDES:
                        for d in gather(a + 4, side):
                            d.start()

            @pl.when(c == 5)
            def _():
                for k in (4, 5):
                    for side in SIDES:
                        for d in gather(k, side):
                            d.wait_send()
                for d in again:
                    d.start()

        step(i + 1, 1)

        @pl.when(fresh & (nxt < 8 * NI))
        def _():
            for a in range(1, 7):
                @pl.when(c - 1 == a)
                def _():
                    if a > 4:
                        for side in SIDES:
                            partial(a - 2, side).wait_recv()
                        ys[a - 4] += rel[a - 5]
                    for h in range(1 + a // 5):
                        for side in SIDES:
                            partial(a, side, h).start()
                if a < 4:
                    @pl.when(c == a + 4)
                    def _():
                        for side in SIDES:
                            partial(a, side).wait_send()
            gates(c)

    BLK = Q // 2
    staged = {}

    def stage(t, dst, src, k):
        d = pltpu.make_async_copy(src, dst, vsem.at[k])
        d.start()
        staged[t] = d

    def early(q):
        return fin.at[q // 2, pl.ds((q % 2) * Q, Q)]

    def home(q):
        return (0, 3)[q // 2], 1 + q // 2, (q % 2) * Q

    def finish(q, h):
        y, x, r0 = home(q)
        rows = pl.ds(r0 + h * BLK, BLK)
        z = ys[y, rows] + lat[q // 2, rows]
        r = z * lax.rsqrt(jnp.mean(z * z, axis=-1, keepdims=True) + EPS) * post[...]
        xr[5 + q // 2, rows] = (xr[x, rows].astype(f32) + r).astype(bf16)
        co = pltpu.make_async_copy(xr.at[5 + q // 2, rows], out.at[pl.ds(q * Q + h * BLK, BLK)], osem.at[2 * q + h])
        co.start()
        return co

    for c in (1, 2):
        for side in SIDES:
            partial(c, side).wait_recv()
    bufs = {0: u0.at[lo_h, pl.ds(0, D)], 2: u0.at[hi_h, pl.ds(0, D)], 1: u1.at[lo_h, pl.ds(0, D)], 3: u1.at[hi_h, pl.ds(0, D)]}
    for q in range(4):
        stage(q, bufs[q], early(q), q)
    for q in range(4):
        staged[q].wait()
        y, x, r0 = home(q)
        ys[y, pl.ds(r0, Q)] += bufs[q][...]
    for d in again:
        d.wait()
    done = []
    for half_q, c in ((0, 5), (1, 6)):
        for h in range(2):
            for side in SIDES:
                partial(c, side, h).wait_recv()
            for q in (half_q, half_q + 2):
                done.append(finish(q, h))
    for k in range(4):
        for side in SIDES:
            for d in gather(k, side):
                d.wait_send()
    for k in range(NI):
        for d in weight(k):
            d.wait_send()
    for c in (4, 5, 6):
        for h in range(1 + c // 5):
            for side in SIDES:
                partial(c, side, h).wait_send()
    for d in done:
        d.wait()


def move(src, dst, buf, si, so):
    n, r = buf.shape[:2]
    ins = [pltpu.make_async_copy(src.at[pl.ds(k * r, r)], buf.at[k], si.at[k]) for k in range(n)]
    outs = [pltpu.make_async_copy(buf.at[k], dst.at[pl.ds(k * r, r)], so.at[k]) for k in range(n)]
    for d in ins:
        d.start()
    for k in range(n):
        ins[k].wait()
        outs[k].start()
    for d in outs:
        d.wait()


def pairs(w):
    e, d, h = w.shape
    return w.transpose(0, 2, 1).reshape(e // 2, 2 * h, d)


def solution(mesh):
    n = mesh.shape['wg']

    def local_block(hidden, choice, pre_scale, w_router, w_gelu, w_linear, w_down, post_scale):
        R, D = hidden.shape
        E, _, H = w_gelu.shape
        K = choice.shape[1]
        M = R // 2
        wd_own = w_down.reshape(E // 2, 2 * H, D)
        cht = choice.T
        any_spec = pl.BlockSpec(memory_space=pl.ANY)
        vmem = pl.BlockSpec(memory_space=pltpu.VMEM)
        sem = pltpu.SemaphoreType.DMA
        out, _ = pl.pallas_call(
            functools.partial(kernel, n),
            out_shape=[jax.ShapeDtypeStruct((R, D), bf16), jax.ShapeDtypeStruct((2, M, D), f32)],
            in_specs=[any_spec, vmem, vmem, vmem, any_spec, any_spec, any_spec, vmem],
            out_specs=[any_spec, any_spec],
            scratch_shapes=[
                pltpu.VMEM((E // 2, 2, 4 * H, D), bf16), pltpu.VMEM((E // 2, 2, 2 * H, D), bf16),
                pltpu.VMEM((8, M, D), bf16), pltpu.VMEM((8, K, M), bf16),
                pltpu.VMEM((M, 3 * E), bf16), pltpu.VMEM((E // SB, 3 * E, SB // 2 * LANES), bf16),
                pltpu.VMEM((M, 256 * SB), f32), pltpu.VMEM((M, 256 * SB), f32),
                pltpu.VMEM((M, 128 * SB), bf16), pltpu.VMEM((M, 128 * SB), bf16),
                pltpu.VMEM((M, 128 * SB), bf16), pltpu.VMEM((M, 128 * SB), bf16),
                pltpu.VMEM((5, M, D), f32), pltpu.VMEM((2, M, D), f32), pltpu.VMEM((2, M, D), f32),
                sem((4,)), sem((24,)), sem((24,)), sem((3 * E // SB,)), sem((3 * E // SB,)), sem((3 * E // SB,)), sem((24,)), sem((24,)), sem((8,))],
            compiler_params=pltpu.CompilerParams(collective_id=0, has_side_effects=True, vmem_limit_bytes=67043328),
        )(hidden, cht, pre_scale.reshape(1, D), w_router.T, pairs(w_gelu), pairs(w_linear), wd_own, post_scale.reshape(1, D))
        parts = 8
        return pl.pallas_call(
            move, out_shape=jax.ShapeDtypeStruct((R, D), bf16), in_specs=[any_spec], out_specs=any_spec,
            scratch_shapes=[pltpu.VMEM((parts, R // parts, D), bf16), sem((parts,)), sem((parts,))])(out)

    row_spec = P(('dp', 'wg'), None)
    weight_in = P(None, None, 'wg')
    return jax.shard_map(local_block, mesh=mesh, in_specs=(row_spec, row_spec, P(), P(), weight_in, weight_in, P(None, 'wg', None), P()), out_specs=row_spec, check_vma=False)
```
